16 devices in a mesh: data: 2 (over y, z), seq: 8 (over x, core).
Axes of the slice: x: 4, y: 2, z: 1, core: 2. Of those that a mesh axis runs over, the one named last changes fastest.
The devices are a block of a 4x4x8 slice.
Arguments:
- tokens: bfloat16 [32, 4096, 1280], P('data', 'seq'), parts along dimension 0
- lengths: int32 [32], P('data'), parts along dimension 0
- slot_params: bfloat16 [1280, 128], replicated
- logit_scale: float32 [1], replicated
- w_in: bfloat16 [32, 1280, 5120], P('seq')
- w_out: bfloat16 [32, 5120, 1280], P('seq')
Outputs:
- output: bfloat16 [32, 4096, 1280], P('data', 'seq'), parts along dimension 0
There are 2 independent parts. The reference program is written for one: setup_inputs(seed, part) draws one part's arguments, and reference() takes and returns one part's arrays. A program takes and returns all parts, laid end to end along the dimension named above; an argument that names none is the same for every part.
All inputs are finite; a program needn't handle non-finite values.
Results may differ from the reference program's by a relative error of at most 0.0155195.
Values are sent between devices in bfloat16 or wider.
A program may use at most 768 MiB of HBM per device.

```python
import jax
import jax.numpy as jnp
from jax import lax

BATCH = 16
TOKENS = 4096
D_MODEL = 1280
FF_DIM = 5120
EXPERTS = 32
SLOTS = 4
NUM_SLOTS = EXPERTS * SLOTS


def setup_inputs(seed: int = 0, part: int = 0) -> dict:
    base_key = jax.random.key(seed)
    k_phi, k_win, k_wout, k_gain = jax.random.split(base_key, 4)
    part_key = jax.random.fold_in(base_key, part)
    k_sel, k_noise, k_len = jax.random.split(part_key, 3)
    slot_params = jax.random.normal(k_phi, (D_MODEL, NUM_SLOTS), jnp.float32)
    chosen = jax.random.randint(k_sel, (BATCH, TOKENS), 0, NUM_SLOTS)
    noise = jax.random.normal(k_noise, (BATCH, TOKENS, D_MODEL), jnp.float32)
    tokens = jnp.take(slot_params.T, chosen, axis=0) + noise
    lengths = jax.random.randint(k_len, (BATCH,), 1, TOKENS + 1)
    logit_scale = jax.random.uniform(k_gain, (1,), jnp.float32, 6.0, 9.0)
    w_in = jax.random.normal(k_win, (EXPERTS, D_MODEL, FF_DIM), jnp.float32) * D_MODEL ** -0.5
    w_out = jax.random.normal(k_wout, (EXPERTS, FF_DIM, D_MODEL), jnp.float32) * FF_DIM ** -0.5
    return {
        "tokens": tokens.astype(jnp.bfloat16),
        "lengths": lengths.astype(jnp.int32),
        "slot_params": slot_params.astype(jnp.bfloat16),
        "logit_scale": logit_scale,
        "w_in": w_in.astype(jnp.bfloat16),
        "w_out": w_out.astype(jnp.bfloat16),
    }


def reference(tokens, lengths, slot_params, logit_scale, w_in, w_out):
    params_f32 = slot_params.astype(jnp.float32)
    col_inv = lax.rsqrt(jnp.sum(params_f32 * params_f32, axis=0, keepdims=True) + 1e-6)
    phi_norm = (params_f32 * (logit_scale[0] * col_inv)).astype(jnp.bfloat16)
    positions = jnp.arange(TOKENS)

    def row_logits(row_tokens):
        tok_f32 = row_tokens.astype(jnp.float32)
        tok_norm = (tok_f32 * lax.rsqrt(jnp.sum(tok_f32 * tok_f32, axis=-1, keepdims=True) + 1e-6)).astype(jnp.bfloat16)
        return jnp.dot(tok_norm, phi_norm, preferred_element_type=jnp.float32)

    def dispatch_row(row_args):
        row_tokens, row_len = row_args
        logits = row_logits(row_tokens)
        is_valid = (positions < row_len)[:, None]
        col_max = jnp.max(jnp.where(is_valid, logits, -jnp.inf), axis=0)
        disp_w = jnp.where(is_valid, jnp.exp(logits - col_max[None, :]), 0.0)
        col_sum = jnp.sum(disp_w, axis=0)
        slot_sum = jnp.dot(disp_w.astype(jnp.bfloat16).T, row_tokens, preferred_element_type=jnp.float32)
        return (slot_sum / col_sum[:, None]).astype(jnp.bfloat16)

    slot_in = lax.map(dispatch_row, (tokens, lengths))
    by_expert = slot_in.reshape(BATCH, EXPERTS, SLOTS, D_MODEL).transpose(1, 0, 2, 3).reshape(EXPERTS, BATCH * SLOTS, D_MODEL)

    def expert_ffn(exp_args):
        exp_in, exp_w_in, exp_w_out = exp_args
        hidden = jax.nn.gelu(jnp.dot(exp_in, exp_w_in, preferred_element_type=jnp.float32)).astype(jnp.bfloat16)
        return jnp.dot(hidden, exp_w_out, preferred_element_type=jnp.float32).astype(jnp.bfloat16)

    expert_out = lax.map(expert_ffn, (by_expert, w_in, w_out))
    slot_out = expert_out.reshape(EXPERTS, BATCH, SLOTS, D_MODEL).transpose(1, 0, 2, 3).reshape(BATCH, NUM_SLOTS, D_MODEL)

    def combine_row(row_args):
        row_tokens, row_len, row_slots = row_args
        logits = row_logits(row_tokens)
        is_valid = (positions < row_len)[:, None]
        combine_w = jax.nn.softmax(logits, axis=-1).astype(jnp.bfloat16)
        mixed = jnp.dot(combine_w, row_slots, preferred_element_type=jnp.float32).astype(jnp.bfloat16)
        return jnp.where(is_valid, mixed, jnp.zeros_like(mixed))

    return lax.map(combine_row, (tokens, lengths, slot_out))
```

```python
import functools

import jax
import jax.numpy as jnp
from jax import lax
from jax.experimental import pallas as pl
from jax.experimental.pallas import tpu as pltpu
from jax.sharding import PartitionSpec as P

MESH = pl.DeviceIdType.MESH
F32, BF16 = jnp.float32, jnp.bfloat16
TOK_SLOTS = 4
W_SLOTS = 14
F_BLOCK = 512
ROW_TILE = 128


def iota(shape, dim):
    return lax.broadcasted_iota(jnp.int32, shape, dim)


def route_kernel(
    lens, gain, phi, tok, w_in, w_out, c_out, y_out,
    tok_buf, phin, wt_buf, s_f32, c_buf, part, from_partner, relay_r, relay_l, from_l, from_r, xs, z_own, z_all,
    xk, y_acc, ys, wi_buf, wo_buf,
    tok_sem, wi_sem, wo_sem, c_sem, yo_sem, z_send, z_recv,
    d_send, d_recv, rs_send, rs_recv, ag_send, ag_recv,
):
    rows, tokens, width = tok.shape
    experts, _, ff = w_in.shape
    slots = phi.shape[1]
    pairs = rows // 2
    blocks = ff // F_BLOCK
    steps = experts * blocks
    me = lax.axis_index("seq")
    chip, core = me // 2, lax.rem(me, 2)

    def dev(chip_step, flip=0):
        other = lax.rem(chip + chip_step, 4)
        return other * 2 + (1 - core if flip else core)

    left, right, opposite, partner = dev(3), dev(1), dev(2), dev(0, 1)
    c_left, c_right, c_opp = lax.rem(chip + 3, 4), lax.rem(chip + 1, 4), lax.rem(chip + 2, 4)

    barrier = pltpu.get_barrier_semaphore()
    for step in range(1, 8):
        peer = lax.rem(me + step, 8)
        pl.semaphore_signal(barrier, inc=1, device_id={"seq": peer}, device_id_type=MESH)

    def tok_copy(b):
        slot = lax.rem(b, TOK_SLOTS)
        return pltpu.make_async_copy(tok.at[b], tok_buf.at[slot], tok_sem.at[slot])

    def w_copies(i):
        e, f, slot = i // blocks, lax.rem(i, blocks), lax.rem(i, W_SLOTS)
        cols = pl.ds(pl.multiple_of(f * F_BLOCK, F_BLOCK), F_BLOCK)
        return (
            pltpu.make_async_copy(w_in.at[e, :, cols], wi_buf.at[slot], wi_sem.at[slot]),
            pltpu.make_async_copy(w_out.at[e, cols, :], wo_buf.at[slot], wo_sem.at[slot]),
        )

    for b in range(TOK_SLOTS):
        tok_copy(b).start()

    gain_s = gain[0]
    phi_f32 = phi[...].astype(F32)
    col_inv = lax.rsqrt(jnp.sum(phi_f32 * phi_f32, axis=0, keepdims=True) + 1e-6)
    phi_n = (phi_f32 * (gain_s * col_inv)).astype(BF16)
    src, dst = iota((slots, slots), 0), iota((slots, slots), 1)
    kk, hh, cc, rest = dst // 64, (dst // 32) % 2, (dst // 8) % 4, dst % 8
    perm = (src == cc * 32 + hh * 16 + kk * 8 + rest).astype(F32).astype(BF16)
    phin[...] = jnp.dot(phi_n, perm, preferred_element_type=F32).astype(BF16)

    def one_batch(b, which):
        slot = lax.rem(b, TOK_SLOTS)
        tok_copy(b).wait()
        x_ref = tok_buf.at[slot]
        length = lens[b]
        z_row = jnp.zeros((1, slots), F32)
        for r in range(tokens // ROW_TILE):
            tile = pl.ds(r * ROW_TILE, ROW_TILE)
            x = x_ref[tile, :].astype(F32)
            inv = lax.rsqrt(jnp.sum(x * x, axis=-1, keepdims=True) + 1e-6)
            logits = jnp.dot((x * inv).astype(BF16), phin[...], preferred_element_type=F32)
            e = jnp.exp(logits - gain_s)
            pos = me * tokens + r * ROW_TILE + iota((ROW_TILE, slots), 0)
            valid = pos < length
            total = jnp.sum(e, axis=-1, keepdims=True)
            c_buf[b, tile, :] = jnp.where(valid, e / total, 0.0).astype(BF16)
            w = jnp.where(valid, e, 0.0)
            z_row += jnp.sum(w, axis=0, keepdims=True)
            wt_buf[:, tile] = w.T.astype(BF16)
        z_own[pl.ds(b, 1), :] = z_row
        s_f32[which] = jnp.dot(wt_buf[...], x_ref[...], preferred_element_type=F32)

        @pl.when(b + TOK_SLOTS < rows)
        def _():
            tok_copy(b + TOK_SLOTS).start()

        @pl.when(b < W_SLOTS)
        def _():
            for copy in w_copies(b):
                copy.start()

    def one_pair(p, carry):
        for which in range(2):
            one_batch(2 * p + which, which)
        for g in range(16):
            eight = pl.ds(g * 8, 8)
            both = jnp.concatenate([s_f32[0, eight, :], s_f32[1, eight, :]], axis=0)
            part[g // 8, (g // 4) % 2, g % 4, p] = both.astype(BF16)
        return carry

    def remote(src_ref, dst_ref, send, recv, to):
        return pltpu.make_async_remote_copy(
            src_ref=src_ref, dst_ref=dst_ref, send_sem=send, recv_sem=recv, device_id={"seq": to}, device_id_type=MESH
        )

    def d2d(kk, q):
        two = pl.ds(2 * q, 2)
        return remote(part.at[kk, 1 - core, :, two], from_partner.at[kk, :, two], d_send.at[kk, q], d_recv.at[kk, q], partner)

    def rs_copy(kind, kk, q):
        plus, minus = 2 * q, 2 * q + 1
        mine = part.at[kk, core]
        src_ref, dst_ref, to = {
            "ap": (mine.at[c_opp, plus], relay_r.at[kk, q], right),
            "am": (mine.at[c_opp, minus], relay_l.at[kk, q], left),
            "bp0": (mine.at[c_right, minus], from_l.at[kk, minus], right),
            "bm0": (mine.at[c_left, plus], from_r.at[kk, plus], left),
            "bp1": (mine.at[c_right, plus], from_l.at[kk, plus], right),
            "bm1": (mine.at[c_left, minus], from_r.at[kk, minus], left),
        }[kind]
        n = ("ap", "am", "bp0", "bm0", "bp1", "bm1").index(kind)
        return remote(src_ref, dst_ref, rs_send.at[n, kk, q], rs_recv.at[n, kk, q], to)

    def s2(kk, q):
        d2d(kk, q).wait_recv()
        for c in range(4):
            for p in (2 * q, 2 * q + 1):
                total = part[kk, core, c, p].astype(F32) + from_partner[kk, c, p].astype(F32)
                part[kk, core, c, p] = total.astype(BF16)
        for kind in ("ap", "am", "bp0", "bm0"):
            rs_copy(kind, kk, q).start()

    def s3(kk, q):
        rs_copy("ap", kk, q).wait_recv()
        plus, minus = 2 * q, 2 * q + 1
        part[kk, core, c_right, plus] = (
            part[kk, core, c_right, plus].astype(F32) + relay_r[kk, q].astype(F32)
        ).astype(BF16)
        rs_copy("bp1", kk, q).start()
        rs_copy("am", kk, q).wait_recv()
        part[kk, core, c_left, minus] = (
            part[kk, core, c_left, minus].astype(F32) + relay_l[kk, q].astype(F32)
        ).astype(BF16)
        rs_copy("bm1", kk, q).start()

    def s4(kk):
        lane0 = kk * 64 + core * 32 + chip * 8
        pick = iota((16, slots), 1) == lane0 + iota((16, slots), 0) % 8
        for q in range(4):
            for kind in ("bp0", "bm0", "bp1", "bm1"):
                rs_copy(kind, kk, q).wait_recv()
            for p in (2 * q, 2 * q + 1):
                z = z_own[2 * p : 2 * p + 2, :]
                for step in range(1, 8):
                    z += z_all[lax.rem(me + step, 8), 2 * p : 2 * p + 2, :]
                z16 = jnp.concatenate([jnp.broadcast_to(z[i : i + 1], (8, slots)) for i in range(2)], axis=0)
                z_col = jnp.sum(jnp.where(pick, z16, 0.0), axis=1, keepdims=True)
                total = part[kk, core, chip, p].astype(F32) + from_l[kk, p].astype(F32) + from_r[kk, p].astype(F32)
                xs[kk, p] = (total / z_col).astype(BF16)

    def z_copy(step):
        peer = lax.rem(me + step, 8)
        return remote(z_own, z_all.at[me], z_send.at[step - 1], z_recv.at[step - 1], peer)

    def chunk(q):
        lax.fori_loop(2 * q, 2 * q + 2, one_pair, 0)

    chunk(0)
    pl.semaphore_wait(barrier, 7)
    for q in range(4):
        if q:
            chunk(q)
        d2d(0, q).start()
        d2d(1, q).start()
        if q >= 1:
            s2(0, q - 1)
        if q >= 2:
            s3(0, q - 2)
    for step in range(1, 8):
        z_copy(step).start()
    c_copy = pltpu.make_async_copy(c_buf, c_out, c_sem)
    c_copy.start()
    s2(0, 3)
    s3(0, 2)
    s2(1, 0)
    s3(0, 3)
    s2(1, 1)
    for step in range(1, 8):
        z_copy(step).wait_recv()
    s2(1, 2)
    s3(1, 0)
    s4(0)

    half = 2 * rows
    lo, hi = pl.ds(0, half), pl.ds(half, half)

    def ag_copy(kind, k):
        blk = ys.at[k]
        src_blk, part_rows, to = {
            "rp": (me, lo, right),
            "lm": (me, hi, left),
            "rm": (me, hi, right),
            "lp": (me, lo, left),
            "fr": (left, lo, right),
            "fl": (right, hi, left),
            "po": (me, None, partner),
            "pl": (left, None, partner),
            "pr": (right, None, partner),
            "pp": (opposite, None, partner),
        }[kind]
        n = ("rp", "lm", "rm", "lp", "fr", "fl", "po", "pl", "pr", "pp").index(kind)
        ref = blk.at[src_blk] if part_rows is None else blk.at[src_blk, part_rows]
        return remote(ref, ref, ag_send.at[n, k], ag_recv.at[n, k], to)

    def a1(k):
        for kind in ("rp", "lm", "rm", "lp", "po"):
            ag_copy(kind, k).start()

    def a2(k):
        ag_copy("rp", k).wait_recv()
        ag_copy("fr", k).start()
        ag_copy("lm", k).wait_recv()
        ag_copy("fl", k).start()

    def a3(k):
        ag_copy("rm", k).wait_recv()
        ag_copy("pl", k).start()
        ag_copy("lp", k).wait_recv()
        ag_copy("pr", k).start()

    def a4(k):
        ag_copy("fr", k).wait_recv()
        ag_copy("fl", k).wait_recv()
        ag_copy("pp", k).start()

    def y_copy(k):
        return pltpu.make_async_copy(ys.at[k], y_out.at[k], yo_sem.at[k])

    def a5(k):
        for kind in ("po", "pl", "pr", "pp"):
            ag_copy(kind, k).wait_recv()
        y_copy(k).start()

    hooks = {
        0: [lambda: s2(1, 3)],
        1: [lambda: s3(1, 1)],
        3: [lambda: s3(1, 2)],
        5: [lambda: s3(1, 3)],
        14: [lambda: a2(0)],
        17: [lambda: a3(0)],
        19: [lambda: s4(1)],
        22: [lambda: a4(0)],
        24: [lambda: a2(1)],
        26: [lambda: a5(0), lambda: a3(1)],
        32: [lambda: a4(1)],
        34: [lambda: a2(2)],
        36: [lambda: a5(1), lambda: a3(2)],
    }

    def ffn_step(i, carry):
        k, f, slot = i // blocks, lax.rem(i, blocks), lax.rem(i, W_SLOTS)

        @pl.when(f == 0)
        def _():
            k2 = lax.rem(k, 2)
            r, c = iota((4 * rows, 8 * rows), 0), iota((4 * rows, 8 * rows), 1)
            sel = (c == (r // 4) * 8 + k2 * 4 + r % 4).astype(F32).astype(BF16)
            pair = xs[k // 2].reshape(8 * rows, width)
            xk[...] = jnp.dot(sel, pair, preferred_element_type=F32).astype(BF16)
            y_acc[...] = jnp.zeros_like(y_acc)

        wi, wo = w_copies(i)
        wi.wait()
        h = jnp.dot(xk[...], wi_buf[slot], preferred_element_type=F32)
        h = jax.nn.gelu(h).astype(BF16)
        wo.wait()
        y_acc[...] += jnp.dot(h, wo_buf[slot], preferred_element_type=F32)

        @pl.when(i + W_SLOTS < steps)
        def _():
            for copy in w_copies(i + W_SLOTS):
                copy.start()

        for at, todo in hooks.items():
            @pl.when(i == at)
            def _(todo=todo):
                for hook in todo:
                    hook()

        @pl.when(f == blocks - 1)
        def _():
            ys[k, me] = y_acc[...].astype(BF16)
            a1(k)

        return carry

    lax.fori_loop(0, steps, ffn_step, 0)
    a4(2)
    a2(3)
    a5(2)
    a3(3)
    a4(3)
    a5(3)

    c_copy.wait()
    for k in range(4):
        y_copy(k).wait()
    for step in range(1, 8):
        z_copy(step).wait_send()
    for kk in range(2):
        for q in range(4):
            d2d(kk, q).wait_send()
            for kind in ("ap", "am", "bp0", "bm0", "bp1", "bm1"):
                rs_copy(kind, kk, q).wait_send()
    for k in range(4):
        for kind in ("rp", "lm", "rm", "lp", "fr", "fl", "po", "pl", "pr", "pp"):
            ag_copy(kind, k).wait_send()


def combine_kernel(c_ref, y_ref, out_ref):
    experts, devs, eight, width = y_ref.shape
    slots = c_ref.shape[2]
    r = y_ref[...].reshape(experts * devs, eight, width).astype(F32).reshape(experts * devs * eight, width).astype(BF16)
    col, row = iota((slots, 2 * slots), 0), iota((slots, 2 * slots), 1)
    kk, core, chip, k2, s = col // 64, (col // 32) % 2, (col // 8) % 4, (col // 4) % 2, col % 4
    base = (kk * 2 + k2) * 64 + (chip * 2 + core) * 8 + s
    for which in range(2):
        spread = (row == base + which * 4).astype(F32).astype(BF16)
        c = jnp.dot(c_ref[which], spread, preferred_element_type=F32).astype(BF16)
        out_ref[which] = jnp.dot(c, r, preferred_element_type=F32).astype(BF16)


def solution(mesh):
    def shard_body(tok, lens, phi, gain, w_in, w_out):
        rows, tokens, width = tok.shape
        experts, _, ff = w_in.shape
        slots = phi.shape[1]
        pairs = rows // 2
        any_spec = pl.BlockSpec(memory_space=pl.ANY)
        smem = pl.BlockSpec(memory_space=pltpu.SMEM)
        dma = pltpu.SemaphoreType.DMA
        blk = (16, width)
        c, y = pl.pallas_call(
            route_kernel,
            out_shape=(
                jax.ShapeDtypeStruct((rows, tokens, slots), BF16),
                jax.ShapeDtypeStruct((experts, 8, 4 * rows, width), BF16),
            ),
            in_specs=[smem, smem, pl.BlockSpec(memory_space=pltpu.VMEM), any_spec, any_spec, any_spec],
            out_specs=(any_spec, any_spec),
            scratch_shapes=[
                pltpu.VMEM((TOK_SLOTS, tokens, width), BF16),
                pltpu.VMEM((width, slots), BF16),
                pltpu.VMEM((slots, tokens), BF16),
                pltpu.VMEM((2, slots, width), F32),
                pltpu.VMEM((rows, tokens, slots), BF16),
                pltpu.VMEM((2, 2, 4, pairs) + blk, BF16),
                pltpu.VMEM((2, 4, pairs) + blk, BF16),
                pltpu.VMEM((2, 4) + blk, BF16),
                pltpu.VMEM((2, 4) + blk, BF16),
                pltpu.VMEM((2, pairs) + blk, BF16),
                pltpu.VMEM((2, pairs) + blk, BF16),
                pltpu.VMEM((2, pairs) + blk, BF16),
                pltpu.VMEM((rows, slots), F32),
                pltpu.VMEM((8, rows, slots), F32),
                pltpu.VMEM((4 * rows, width), BF16),
                pltpu.VMEM((4 * rows, width), F32),
                pltpu.VMEM((experts, 8, 4 * rows, width), BF16),
                pltpu.VMEM((W_SLOTS, width, F_BLOCK), BF16),
                pltpu.VMEM((W_SLOTS, F_BLOCK, width), BF16),
                dma((TOK_SLOTS,)), dma((W_SLOTS,)), dma((W_SLOTS,)), dma, dma((4,)), dma((7,)), dma((7,)),
                dma((2, 4)), dma((2, 4)), dma((6, 2, 4)), dma((6, 2, 4)), dma((10, 4)), dma((10, 4)),
            ],
            compiler_params=pltpu.CompilerParams(
                collective_id=0, has_side_effects=True, vmem_limit_bytes=67_000_000
            ),
            name="route",
        )(lens, gain, phi, tok, w_in, w_out)
        return pl.pallas_call(
            combine_kernel,
            out_shape=jax.ShapeDtypeStruct(tok.shape, BF16),
            grid=(pairs,),
            in_specs=[
                pl.BlockSpec((2, tokens, slots), lambda p: (p, 0, 0)),
                pl.BlockSpec((experts, 8, 8, width), lambda p: (0, 0, p, 0)),
            ],
            out_specs=pl.BlockSpec((2, tokens, width), lambda p: (p, 0, 0)),
            compiler_params=pltpu.CompilerParams(vmem_limit_bytes=50_000_000),
            name="combine",
        )(c, y)

    return jax.shard_map(
        shard_body,
        mesh=mesh,
        in_specs=(P("data", "seq", None), P("data"), P(None, None), P(None), P("seq", None, None), P("seq", None, None)),
        out_specs=P("data", "seq", None),
        check_vma=False,
    )
```

```python
import functools

import jax
import jax.numpy as jnp
from jax import lax
from jax.experimental import pallas as pl
from jax.experimental.pallas import tpu as pltpu
from jax.sharding import PartitionSpec as P

MESH = pl.DeviceIdType.MESH
F32, BF16 = jnp.float32, jnp.bfloat16
TOK_SLOTS = 4
W_SLOTS = 6
F_BLOCK = 1280
ROW_TILE = 128


def iota(shape, dim):
    return lax.broadcasted_iota(jnp.int32, shape, dim)


def route_kernel(
    lens, gain, phi, tok, w_in, w_out, c_out, y_out,
    tok_buf, phin, wt_buf, s_f32, c_buf, part, from_partner, relay_r, relay_l, from_l, from_r, from_opp, xs, z_own, z_all, z_tot,
    xk, h_buf, y_acc, ys, wi_buf, wo_buf,
    tok_sem, wi_sem, wo_sem, c_sem, yo_sem, z_send, z_recv,
    d_send, d_recv, a_send, a_recv, b_send, b_recv, o_send, o_recv, ag_send, ag_recv,
):
    rows, tokens, width = tok.shape
    experts, _, ff = w_in.shape
    slots = phi.shape[1]
    pairs = rows // 2
    blocks = ff // F_BLOCK
    steps = experts * blocks
    me = lax.axis_index("seq")
    chip, core = me // 2, lax.rem(me, 2)

    def dev(chip_step, flip=0):
        other = lax.rem(chip + chip_step, 4)
        return other * 2 + (1 - core if flip else core)

    left, right, opposite, partner = dev(3), dev(1), dev(2), dev(0, 1)
    c_left, c_right, c_opp = lax.rem(chip + 3, 4), lax.rem(chip + 1, 4), lax.rem(chip + 2, 4)

    barrier = pltpu.get_barrier_semaphore()
    for step in range(1, 8):
        peer = lax.rem(me + step, 8)
        pl.semaphore_signal(barrier, inc=1, device_id={"seq": peer}, device_id_type=MESH)

    def tok_copy(b):
        slot = lax.rem(b, TOK_SLOTS)
        return pltpu.make_async_copy(tok.at[b], tok_buf.at[slot], tok_sem.at[slot])

    def w_copies(i):
        e, f, slot = i // blocks, lax.rem(i, blocks), lax.rem(i, W_SLOTS)
        cols = pl.ds(pl.multiple_of(f * F_BLOCK, F_BLOCK), F_BLOCK)
        return (
            pltpu.make_async_copy(w_in.at[e, :, cols], wi_buf.at[slot], wi_sem.at[slot]),
            pltpu.make_async_copy(w_out.at[e, cols, :], wo_buf.at[slot], wo_sem.at[slot]),
        )

    for b in range(TOK_SLOTS):
        tok_copy(b).start()

    gain_s = gain[0]
    phi_f32 = phi[...].astype(F32)
    col_inv = lax.rsqrt(jnp.sum(phi_f32 * phi_f32, axis=0, keepdims=True) + 1e-6)
    phi_n = (phi_f32 * (gain_s * col_inv)).astype(BF16)
    src, dst = iota((slots, slots), 0), iota((slots, slots), 1)
    kk, hh, cc, rest = dst // 64, (dst // 32) % 2, (dst // 8) % 4, dst % 8
    perm = (src == cc * 32 + hh * 16 + kk * 8 + rest).astype(F32).astype(BF16)
    phin[...] = jnp.dot(phi_n, perm, preferred_element_type=F32).astype(BF16)

    def c_copy(p):
        slot = lax.rem(p, 2)
        return pltpu.make_async_copy(c_buf.at[slot], c_out.at[pl.ds(2 * p, 2)], c_sem.at[slot])

    def pack_pair(p):
        for g in range(16):
            eight = pl.ds(g * 8, 8)
            both = jnp.concatenate([s_f32[0, eight, :], s_f32[1, eight, :]], axis=0)
            part[g // 8, (g // 4) % 2, g % 4, p] = both.astype(BF16)

    def one_pair(p):
        for which in range(2):
            b = 2 * p + which
            x_ref = tok_buf.at[lax.rem(b, TOK_SLOTS)]
            length = lens[b]
            z_row = jnp.zeros((1, slots), F32)
            for r in range(tokens // ROW_TILE):
                tile = pl.ds(r * ROW_TILE, ROW_TILE)
                x = x_ref[tile, :].astype(F32)
                inv = lax.rsqrt(jnp.sum(x * x, axis=-1, keepdims=True) + 1e-6)
                logits = jnp.dot((x * inv).astype(BF16), phin[...], preferred_element_type=F32)
                e = jnp.exp(logits - gain_s)
                pos = me * tokens + r * ROW_TILE + iota((ROW_TILE, slots), 0)
                valid = pos < length
                total = jnp.sum(e, axis=-1, keepdims=True)
                c_buf[lax.rem(p, 2), which, tile, :] = jnp.where(valid, e / total, 0.0).astype(BF16)
                w = jnp.where(valid, e, 0.0)
                z_row += jnp.sum(w, axis=0, keepdims=True)
                wt_buf[which, :, tile] = w.T.astype(BF16)
            z_own[pl.ds(b, 1), :] = z_row
            s_f32[which] = jnp.dot(wt_buf[which], x_ref[...], preferred_element_type=F32)
        pack_pair(p)

    def remote(src_ref, dst_ref, send, recv, to):
        return pltpu.make_async_remote_copy(
            src_ref=src_ref, dst_ref=dst_ref, send_sem=send, recv_sem=recv, device_id={"seq": to}, device_id_type=MESH
        )

    lo_cols, hi_cols = pl.ds(0, width // 2), pl.ds(width // 2, width // 2)

    def settle(ref, sem):
        pltpu.make_async_copy(ref, ref, sem).wait()

    def d2d(kk, p):
        return remote(part.at[kk, 1 - core, :, p], from_partner.at[kk, :, p], d_send, d_recv.at[kk, p], partner)

    def rs_copy(kind, kk, p):
        mine = part.at[kk, core]
        to_right = kind[1] == "p"
        side, to = (0, right) if to_right else (1, left)
        if kind[0] == "a":
            cols, relay = (lo_cols, relay_r) if to_right else (hi_cols, relay_l)
            return remote(mine.at[c_opp, p, :, cols], relay.at[kk, p], a_send.at[side, kk], a_recv.at[side, kk, p], to)
        cols = hi_cols if kind in ("bp0", "bm1") else lo_cols
        c, inbox = (c_right, from_l) if to_right else (c_left, from_r)
        return remote(mine.at[c, p, :, cols], inbox.at[kk, p, :, cols], b_send.at[side], b_recv.at[side, kk], to)

    def chip_sum(kk, p):
        d2d(kk, p).wait_recv()
        for c in range(4):
            total = part[kk, core, c, p].astype(F32) + from_partner[kk, c, p].astype(F32)
            part[kk, core, c, p] = total.astype(BF16)

    def s2(kk, p):
        chip_sum(kk, p)
        for kind in ("ap", "am", "bp0", "bm0"):
            rs_copy(kind, kk, p).start()

    def last_copies():
        p = pairs - 1
        mine = part.at[0, core]
        return (
            remote(mine.at[c_opp, p], from_opp, o_send, o_recv, opposite),
            remote(mine.at[c_right, p], from_l.at[0, p], b_send.at[0], b_recv.at[0, 0], right),
            remote(mine.at[c_left, p], from_r.at[0, p], b_send.at[1], b_recv.at[1, 0], left),
        )

    def s2_last():
        chip_sum(0, pairs - 1)
        for copy in last_copies():
            copy.start()

    def s3(kk, p):
        for kind, then, c, relay, cols in (
            ("ap", "bp1", c_right, relay_r, lo_cols),
            ("am", "bm1", c_left, relay_l, hi_cols),
        ):
            rs_copy(kind, kk, p).wait_recv()
            total = part[kk, core, c, p, :, cols].astype(F32) + relay[kk, p].astype(F32)
            part[kk, core, c, p, :, cols] = total.astype(BF16)
            rs_copy(then, kk, p).start()

    def s4(kk):
        lane0 = kk * 64 + core * 32 + chip * 8
        pick = iota((16, slots), 1) == lane0 + iota((16, slots), 0) % 8
        cols = []
        for p in range(pairs):
            z16 = jnp.concatenate([jnp.broadcast_to(z_tot[b : b + 1, :], (8, slots)) for b in (2 * p, 2 * p + 1)], axis=0)
            cols.append(jnp.sum(jnp.where(pick, z16, 0.0), axis=1, keepdims=True))
        settle(from_l.at[kk], b_recv.at[0, kk])
        settle(from_r.at[kk], b_recv.at[1, kk])
        if kk == 0:
            settle(from_opp, o_recv)
        for p in range(pairs):
            total = part[kk, core, chip, p].astype(F32) + from_l[kk, p].astype(F32) + from_r[kk, p].astype(F32)
            if kk == 0 and p == pairs - 1:
                total += from_opp[...].astype(F32)
            xs[kk, p] = (total / cols[p]).astype(BF16)

    def z_copy(step):
        peer = lax.rem(me + step, 8)
        return remote(z_own, z_all.at[me], z_send, z_recv, peer)

    def when(condition, *todo):
        @pl.when(condition)
        def _():
            for f, *args in todo:
                f(*args)

    def pair_step(p, carry):
        when(p >= 2, (lambda: c_copy(p - 2).wait(),))
        for which in range(2):
            tok_copy(2 * p + which).wait()
        one_pair(p)
        d2d(0, p).start()
        d2d(1, p).start()
        c_copy(p).start()
        for which in range(2):
            b = 2 * p + TOK_SLOTS + which
            when(b < rows, (lambda b=b: tok_copy(b).start(),))
        when(p < W_SLOTS, (lambda: [copy.start() for copy in w_copies(p)],))
        odd = lax.rem(p, 2)
        when(p >= 1, (s2, 0, p - 1))
        when(p >= 3, (s3, 0, p - 3))
        when((p >= 4) & (odd == 0), (s3, 1, p // 2 - 2))
        when((p >= 2) & (odd == 0), (s2, 1, p // 2 - 1))
        return carry

    pl.semaphore_wait(barrier, 7)
    lax.fori_loop(0, pairs, pair_step, 0)
    for step in range(1, 8):
        z_copy(step).start()
    s2_last()
    s3(0, pairs - 3)
    s3(0, pairs - 2)
    s3(1, pairs // 2 - 2)
    for p in range(pairs // 2 - 1, pairs):
        s2(1, p)
    settle(z_all.at[pl.ds(0, 7)], z_recv)
    z = z_own[...]
    for step in range(1, 8):
        z += z_all[lax.rem(me + step, 8)]
    z_tot[...] = z
    s4(0)

    half = 2 * rows
    lo, hi = pl.ds(0, half), pl.ds(half, half)

    def ag_copy(kind, k):
        src_blk, part_rows, to, arrival = {
            "rp": (me, lo, right, 0),
            "lm": (me, hi, left, 0),
            "rm": (me, hi, right, 1),
            "lp": (me, lo, left, 1),
            "fr": (left, lo, right, 2),
            "fl": (right, hi, left, 2),
            "po": (me, None, partner, 3),
            "pl": (left, None, partner, 3),
            "pr": (right, None, partner, 3),
            "pp": (opposite, None, partner, 3),
        }[kind]
        ref = ys.at[k, src_blk] if part_rows is None else ys.at[k, src_blk, part_rows]
        return remote(ref, ref, ag_send.at[k], ag_recv.at[arrival, k], to)

    def a1(k):
        for kind in ("rp", "lm", "rm", "lp", "po"):
            ag_copy(kind, k).start()

    def a2(k):
        settle(ys.at[k, left], ag_recv.at[0, k])
        ag_copy("fr", k).start()
        ag_copy("fl", k).start()

    def a3(k):
        settle(ys.at[k, left], ag_recv.at[1, k])
        ag_copy("pl", k).start()
        ag_copy("pr", k).start()

    def a4(k):
        settle(ys.at[k, opposite], ag_recv.at[2, k])
        ag_copy("pp", k).start()

    def a5(k):
        settle(ys.at[k, pl.ds(0, 4)], ag_recv.at[3, k])
        pltpu.make_async_copy(ys.at[k], y_out.at[k], yo_sem).start()

    def select(k):
        k2 = lax.rem(k, 2)
        r, c = iota((4 * rows, 8 * rows), 0), iota((4 * rows, 8 * rows), 1)
        sel = (c == (r // 4) * 8 + k2 * 4 + r % 4).astype(F32).astype(BF16)
        pair = xs[k // 2].reshape(8 * rows, width)
        xk[k2] = jnp.dot(sel, pair, preferred_element_type=F32).astype(BF16)

    def hidden(i):
        x = xk[lax.rem(i // blocks, 2)]
        return jax.nn.gelu(jnp.dot(x, wi_buf[lax.rem(i, W_SLOTS)], preferred_element_type=F32)).astype(BF16)

    hooks = {
        0: [(s3, 1, p) for p in range(pairs // 2 - 1, pairs)] + [(select, 1)],
        2: [(s4, 1), (select, 2)],
        3: [(a2, 0)],
        4: [(a3, 0), (select, 3)],
        5: [(a2, 1)],
        6: [(a3, 1), (a4, 0), (a2, 2)],
    }

    def ffn_step(t, carry):
        i = 2 * t
        k = i // blocks
        after = [i + 1, jnp.minimum(i + 2, steps - 1)]
        w_copies(after[0])[0].wait()
        when(i + 2 < steps, (w_copies(after[1])[0].wait,))
        w_copies(i)[1].wait()
        w_copies(i + 1)[1].wait()
        total = jnp.where(lax.rem(i, blocks) == 0, 0.0, y_acc[...])
        for n in range(2):
            h = hidden(after[n])
            total += jnp.dot(h_buf[n], wo_buf[lax.rem(i + n, W_SLOTS)], preferred_element_type=F32)
            h_buf[1 - n] = h
        y_acc[...] = total
        for n in range(2):
            when(i + n + 1 + W_SLOTS < steps, (w_copies(i + n + 1 + W_SLOTS)[0].start,))
            when(i + n + W_SLOTS < steps, (w_copies(i + n + W_SLOTS)[1].start,))

        @pl.when(lax.rem(i, blocks) == blocks - 2)
        def _():
            ys[k, me] = y_acc[...].astype(BF16)
            a1(k)

        for at, todo in hooks.items():
            when(t == at, *todo)
        return carry

    w_copies(0)[0].wait()
    select(0)
    h_buf[0] = hidden(0)
    w_copies(W_SLOTS)[0].start()
    lax.fori_loop(0, steps // 2, ffn_step, 0)
    a3(2)
    a4(1)
    a5(0)
    a4(2)
    a5(1)
    a2(3)
    a5(2)
    a3(3)
    a4(3)
    a5(3)

    def finish():
        for p in (pairs - 2, pairs - 1):
            c_copy(p).wait()
        pltpu.make_async_copy(ys, y_out, yo_sem).wait()
        settle(z_all.at[pl.ds(0, 7)], z_send)
        settle(from_partner, d_send)
        for side, relay in enumerate((relay_r, relay_l)):
            settle(relay.at[0, pl.ds(0, pairs - 1)], a_send.at[side, 0])
            settle(relay.at[1], a_send.at[side, 1])
        settle(from_opp, o_send)
        settle(from_l, b_send.at[0])
        settle(from_r, b_send.at[1])
        for k in range(4):
            settle(ys.at[k, pl.ds(0, 7)], ag_send.at[k])

    finish()


def combine_kernel(c_ref, y_ref, out_ref):
    experts, devs, eight, width = y_ref.shape
    slots = c_ref.shape[2]
    r = y_ref[...].reshape(experts * devs, eight, width).astype(F32).reshape(experts * devs * eight, width).astype(BF16)
    col, row = iota((slots, 2 * slots), 0), iota((slots, 2 * slots), 1)
    kk, core, chip, k2, s = col // 64, (col // 32) % 2, (col // 8) % 4, (col // 4) % 2, col % 4
    base = (kk * 2 + k2) * 64 + (chip * 2 + core) * 8 + s
    for which in range(2):
        spread = (row == base + which * 4).astype(F32).astype(BF16)
        c = jnp.dot(c_ref[which], spread, preferred_element_type=F32).astype(BF16)
        out_ref[which] = jnp.dot(c, r, preferred_element_type=F32).astype(BF16)


def solution(mesh):
    def shard_body(tok, lens, phi, gain, w_in, w_out):
        rows, tokens, width = tok.shape
        experts, _, ff = w_in.shape
        slots = phi.shape[1]
        pairs = rows // 2
        any_spec = pl.BlockSpec(memory_space=pl.ANY)
        smem = pl.BlockSpec(memory_space=pltpu.SMEM)
        dma = pltpu.SemaphoreType.DMA
        blk = (16, width)
        c, y = pl.pallas_call(
            route_kernel,
            out_shape=(
                jax.ShapeDtypeStruct((rows, tokens, slots), BF16),
                jax.ShapeDtypeStruct((experts, 8, 4 * rows, width), BF16),
            ),
            in_specs=[smem, smem, pl.BlockSpec(memory_space=pltpu.VMEM), any_spec, any_spec, any_spec],
            out_specs=(any_spec, any_spec),
            scratch_shapes=[
                pltpu.VMEM((TOK_SLOTS, tokens, width), BF16),
                pltpu.VMEM((width, slots), BF16),
                pltpu.VMEM((2, slots, tokens), BF16),
                pltpu.VMEM((2, slots, width), F32),
                pltpu.VMEM((2, 2, tokens, slots), BF16),
                pltpu.VMEM((2, 2, 4, pairs) + blk, BF16),
                pltpu.VMEM((2, 4, pairs) + blk, BF16),
                pltpu.VMEM((2, pairs, 16, width // 2), BF16),
                pltpu.VMEM((2, pairs, 16, width // 2), BF16),
                pltpu.VMEM((2, pairs) + blk, BF16),
                pltpu.VMEM((2, pairs) + blk, BF16),
                pltpu.VMEM(blk, BF16),
                pltpu.VMEM((2, pairs) + blk, BF16),
                pltpu.VMEM((rows, slots), F32),
                pltpu.VMEM((8, rows, slots), F32),
                pltpu.VMEM((rows, slots), F32),
                pltpu.VMEM((2, 4 * rows, width), BF16),
                pltpu.VMEM((2, 4 * rows, F_BLOCK), BF16),
                pltpu.VMEM((4 * rows, width), F32),
                pltpu.VMEM((experts, 8, 4 * rows, width), BF16),
                pltpu.VMEM((W_SLOTS, width, F_BLOCK), BF16),
                pltpu.VMEM((W_SLOTS, F_BLOCK, width), BF16),
                dma((TOK_SLOTS,)), dma((W_SLOTS,)), dma((W_SLOTS,)), dma((2,)), dma, dma, dma,
                dma, dma((2, pairs)), dma((2, 2)), dma((2, 2, pairs)), dma((2,)), dma((2, 2)), dma, dma, dma((4,)), dma((4, 4)),
            ],
            compiler_params=pltpu.CompilerParams(
                collective_id=0, has_side_effects=True, vmem_limit_bytes=67_000_000
            ),
            name="route",
        )(lens, gain, phi, tok, w_in, w_out)
        return pl.pallas_call(
            combine_kernel,
            out_shape=jax.ShapeDtypeStruct(tok.shape, BF16),
            grid=(pairs,),
            in_specs=[
                pl.BlockSpec((2, tokens, slots), lambda p: (p, 0, 0)),
                pl.BlockSpec((experts, 8, 8, width), lambda p: (0, 0, p, 0)),
            ],
            out_specs=pl.BlockSpec((2, tokens, width), lambda p: (p, 0, 0)),
            compiler_params=pltpu.CompilerParams(vmem_limit_bytes=67_000_000),
            name="combine",
        )(c, y)

    return jax.shard_map(
        shard_body,
        mesh=mesh,
        in_specs=(P("data", "seq", None), P("data"), P(None, None), P(None), P("seq", None, None), P("seq", None, None)),
        out_specs=P("data", "seq", None),
        check_vma=False,
    )
```

```python
import functools

import jax
import jax.numpy as jnp
from jax import lax
from jax.experimental import pallas as pl
from jax.experimental.pallas import tpu as pltpu
from jax.sharding import PartitionSpec as P

MESH = pl.DeviceIdType.MESH
F32, BF16 = jnp.float32, jnp.bfloat16
TOK_SLOTS = 4
W_SLOTS = 6
O_SLOTS = W_SLOTS + 1
DIRECT = 1
EARLY = 4
F_BLOCK = 1280
ROW_TILE = 128
IN_SLOTS = 3
OUT_SLOTS = 4


def iota(shape, dim):
    return lax.broadcasted_iota(jnp.int32, shape, dim)


def route_kernel(
    lens, gain, phi, tok, w_in, w_out, c_out, y_out,
    phin, wt_buf, s_f32, c_buf, part, from_partner, relay_r, relay_l, from_l, from_r, from_opp, xs, z_own, z_peer, z_chip, z_all, z_tot,
    xk, h_buf, y_acc, ys, wi_buf, wo_buf,
    tok_sem, wi_sem, wo_sem, c_sem, yo_sem, z_send, z_recv,
    d_send, d_recv, a_send, a_recv, b_send, b_recv, o_send, o_recv, ag_send, ag_recv,
):
    rows, tokens, width = tok.shape
    experts, _, ff = w_in.shape
    slots = phi.shape[1]
    pairs = rows // 2
    blocks = ff // F_BLOCK
    steps = experts * blocks
    me = lax.axis_index("seq")
    chip, core = me // 2, lax.rem(me, 2)

    def dev(chip_step, flip=0):
        other = lax.rem(chip + chip_step, 4)
        return other * 2 + (1 - core if flip else core)

    left, right, opposite, partner = dev(3), dev(1), dev(2), dev(0, 1)
    c_left, c_right, c_opp = lax.rem(chip + 3, 4), lax.rem(chip + 1, 4), lax.rem(chip + 2, 4)

    barrier = pltpu.get_barrier_semaphore()
    for step in range(1, 8):
        peer = lax.rem(me + step, 8)
        pl.semaphore_signal(barrier, inc=1, device_id={"seq": peer}, device_id_type=MESH)

    def tok_slot(b):
        first = W_SLOTS * F_BLOCK + lax.rem(b, TOK_SLOTS) * tokens
        return wo_buf.at[pl.ds(pl.multiple_of(first, 256), tokens)]

    def wo_slot(i):
        return wo_buf.at[pl.ds(pl.multiple_of(lax.rem(i, O_SLOTS) * F_BLOCK, 256), F_BLOCK)]

    def tok_copy(b):
        return pltpu.make_async_copy(tok.at[b], tok_slot(b), tok_sem.at[lax.rem(b, TOK_SLOTS)])

    def w_copies(i):
        e, f = i // blocks, lax.rem(i, blocks)
        cols = pl.ds(pl.multiple_of(f * F_BLOCK, F_BLOCK), F_BLOCK)
        i_slot = lax.rem(i, W_SLOTS)
        return (
            pltpu.make_async_copy(w_in.at[e, :, cols], wi_buf.at[i_slot], wi_sem.at[i_slot]),
            pltpu.make_async_copy(w_out.at[e, cols, :], wo_slot(i), wo_sem.at[lax.rem(i, O_SLOTS)]),
        )

    for b in range(TOK_SLOTS):
        tok_copy(b).start()

    gain_s = gain[0]
    phi_f32 = phi[...].astype(F32)
    col_inv = lax.rsqrt(jnp.sum(phi_f32 * phi_f32, axis=0, keepdims=True) + 1e-6)
    phi_n = (phi_f32 * (gain_s * col_inv)).astype(BF16)
    src, dst = iota((slots, slots), 0), iota((slots, slots), 1)
    kk, hh, cc, rest = dst // 64, (dst // 32) % 2, (dst // 8) % 4, dst % 8
    perm = (src == cc * 32 + hh * 16 + kk * 8 + rest).astype(F32).astype(BF16)
    phin[...] = jnp.dot(phi_n, perm, preferred_element_type=F32).astype(BF16)

    def c_copy(p):
        slot = lax.rem(p, 2)
        return pltpu.make_async_copy(c_buf.at[slot], c_out.at[pl.ds(2 * p, 2)], c_sem.at[slot])

    def pack_pair(p):
        for g in range(16):
            eight = pl.ds(g * 8, 8)
            both = jnp.concatenate([s_f32[0, eight, :], s_f32[1, eight, :]], axis=0)
            part[g // 8, (g // 4) % 2, g % 4, p] = both.astype(BF16)

    def one_pair(p):
        for which in range(2):
            b = 2 * p + which
            x_ref = tok_slot(b)
            length = lens[b]
            z_row = jnp.zeros((1, slots), F32)
            for r in range(tokens // ROW_TILE):
                tile = pl.ds(r * ROW_TILE, ROW_TILE)
                x = x_ref[tile, :].astype(F32)
                inv = lax.rsqrt(jnp.sum(x * x, axis=-1, keepdims=True) + 1e-6)
                logits = jnp.dot((x * inv).astype(BF16), phin[...], preferred_element_type=F32)
                e = jnp.exp(logits - gain_s)
                pos = me * tokens + r * ROW_TILE + iota((ROW_TILE, slots), 0)
                valid = pos < length
                total = jnp.sum(e, axis=-1, keepdims=True)
                c_buf[lax.rem(p, 2), which, tile, :] = jnp.where(valid, e / total, 0.0).astype(BF16)
                w = jnp.where(valid, e, 0.0)
                z_row += jnp.sum(w, axis=0, keepdims=True)
                wt_buf[which, :, tile] = w.T.astype(BF16)
            z_own[pl.ds(b, 1), :] = z_row
            s_f32[which] = jnp.dot(wt_buf[which], x_ref[...], preferred_element_type=F32)
        pack_pair(p)

    def remote(src_ref, dst_ref, send, recv, to):
        return pltpu.make_async_remote_copy(
            src_ref=src_ref, dst_ref=dst_ref, send_sem=send, recv_sem=recv, device_id={"seq": to}, device_id_type=MESH
        )

    lo_cols, hi_cols = pl.ds(0, width // 2), pl.ds(width // 2, width // 2)

    def settle(ref, sem):
        pltpu.make_async_copy(ref, ref, sem).wait()

    def d2d(kk, p):
        return remote(part.at[kk, 1 - core, :, p], from_partner.at[kk, :, p], d_send, d_recv.at[kk, p], partner)

    def rs_copy(kind, kk, p):
        mine = part.at[kk, core]
        to_right = kind[1] == "p"
        side, to = (0, right) if to_right else (1, left)
        if kind[0] == "a":
            cols, relay = (lo_cols, relay_r) if to_right else (hi_cols, relay_l)
            return remote(mine.at[c_opp, p, :, cols], relay.at[kk, p], a_send.at[side, kk], a_recv.at[side, kk, p], to)
        cols = hi_cols if kind in ("bp0", "bm1") else lo_cols
        c, inbox = (c_right, from_l) if to_right else (c_left, from_r)
        return remote(mine.at[c, p, :, cols], inbox.at[kk, p, :, cols], b_send.at[side], b_recv.at[side, kk], to)

    def chip_sum(kk, p):
        d2d(kk, p).wait_recv()
        for c in range(4):
            total = part[kk, core, c, p].astype(F32) + from_partner[kk, c, p].astype(F32)
            part[kk, core, c, p] = total.astype(BF16)

    def s2(kk, p):
        chip_sum(kk, p)
        for kind in ("ap", "am", "bp0", "bm0"):
            rs_copy(kind, kk, p).start()

    def s2_direct(p):
        chip_sum(0, p)
        mine = part.at[0, core]
        n = p - (pairs - DIRECT)
        remote(mine.at[c_opp, p], from_opp.at[n], o_send, o_recv, opposite).start()
        remote(mine.at[c_right, p], from_l.at[0, p], b_send.at[0], b_recv.at[0, 0], right).start()
        remote(mine.at[c_left, p], from_r.at[0, p], b_send.at[1], b_recv.at[1, 0], left).start()

    def s3(kk, p):
        for kind, then, c, relay, cols in (
            ("ap", "bp1", c_right, relay_r, lo_cols),
            ("am", "bm1", c_left, relay_l, hi_cols),
        ):
            rs_copy(kind, kk, p).wait_recv()
            total = part[kk, core, c, p, :, cols].astype(F32) + relay[kk, p].astype(F32)
            part[kk, core, c, p, :, cols] = total.astype(BF16)
            rs_copy(then, kk, p).start()

    def s4(kk):
        lane0 = kk * 64 + core * 32 + chip * 8
        pick = iota((16, slots), 1) == lane0 + iota((16, slots), 0) % 8
        cols = []
        for p in range(pairs):
            z16 = jnp.concatenate([jnp.broadcast_to(z_tot[b : b + 1, :], (8, slots)) for b in (2 * p, 2 * p + 1)], axis=0)
            cols.append(jnp.sum(jnp.where(pick, z16, 0.0), axis=1, keepdims=True))
        settle(from_l.at[kk], b_recv.at[0, kk])
        settle(from_r.at[kk], b_recv.at[1, kk])
        if kk == 0:
            settle(from_opp, o_recv)
        for p in range(pairs):
            total = part[kk, core, chip, p].astype(F32) + from_l[kk, p].astype(F32) + from_r[kk, p].astype(F32)
            if kk == 0 and p >= pairs - DIRECT:
                total += from_opp[p - (pairs - DIRECT)].astype(F32)
            xs[kk, p] = (total / cols[p]).astype(BF16)

    def z_pair():
        return remote(z_own, z_peer, z_send.at[0], z_recv.at[0], partner)

    def z_chips():
        return [remote(z_chip, z_all.at[chip], z_send.at[1], z_recv.at[1], to) for to in (right, left, opposite)]

    def when(condition, *todo):
        @pl.when(condition)
        def _():
            for f, *args in todo:
                f(*args)

    def pair_step(p, carry):
        when(p >= 2, (lambda: c_copy(p - 2).wait(),))
        for which in range(2):
            tok_copy(2 * p + which).wait()
        one_pair(p)
        when(p == pairs - 1, (lambda: z_pair().start(),))
        d2d(0, p).start()
        d2d(1, p).start()
        c_copy(p).start()
        for which in range(2):
            b = 2 * p + TOK_SLOTS + which
            when(b < rows, (lambda b=b: tok_copy(b).start(),))
        for n in range(2 * W_SLOTS):
            when(p == n * pairs // (2 * W_SLOTS), (w_copies(n // 2)[n % 2].start,))
        when((p >= 1) & (p <= pairs - DIRECT), (s2, 0, p - 1))
        when(p > pairs - DIRECT, (s2_direct, p - 1))
        when(p >= 3, (s3, 0, p - 3))
        when((p >= 1) & (p <= EARLY), (s2, 1, p - 1))
        when(p >= pairs - EARLY, (s3, 1, p - (pairs - EARLY)))
        return carry

    pl.semaphore_wait(barrier, 7)
    lax.fori_loop(0, pairs, pair_step, 0)
    w_copies(W_SLOTS)[1].start()
    s2_direct(pairs - 1)
    z_pair().wait_recv()
    z_chip[...] = z_own[...] + z_peer[...]
    for copy in z_chips():
        copy.start()
    for p in range(pairs - 3, pairs - DIRECT):
        s3(0, p)
    for p in range(EARLY, pairs):
        s2(1, p)
    settle(z_all.at[pl.ds(0, 3)], z_recv.at[1])
    z = z_chip[...]
    for c in (c_right, c_left, c_opp):
        z += z_all[c]
    z_tot[...] = z
    s4(0)

    half = 2 * rows
    lo, hi = pl.ds(0, half), pl.ds(half, half)

    split = 3 * (width // 5)
    pieces = 2 + experts - 1

    def piece(c):
        if isinstance(c, int) and c >= experts - 1:
            return experts - 1, pl.ds(0, split) if c == experts - 1 else pl.ds(split, width - split)
        return c, pl.ds(0, width)

    def blk_of(c, d, part_rows=pl.ds(0, 4 * rows)):
        k, cols = piece(c)
        return ys.at[k, d, part_rows, cols]

    def ag_copy(kind, c):
        src_blk, part_rows, to, arrival = {
            "rp": (me, lo, right, 0),
            "lm": (me, hi, left, 0),
            "rm": (me, hi, right, 1),
            "lp": (me, lo, left, 1),
            "fr": (left, lo, right, 2),
            "fl": (right, hi, left, 2),
            "po": (me, None, partner, 3),
            "pl": (left, None, partner, 3),
            "pr": (right, None, partner, 3),
            "pp": (opposite, None, partner, 3),
        }[kind]
        ref = blk_of(c, src_blk) if part_rows is None else blk_of(c, src_blk, part_rows)
        return remote(ref, ref, ag_send.at[c], ag_recv.at[arrival, c], to)

    def a1(c):
        for kind in ("rp", "lm", "rm", "lp", "po"):
            ag_copy(kind, c).start()

    def a2(c):
        settle(blk_of(c, left), ag_recv.at[0, c])
        ag_copy("fr", c).start()
        ag_copy("fl", c).start()

    def a3(c):
        settle(blk_of(c, left), ag_recv.at[1, c])
        ag_copy("pl", c).start()
        ag_copy("pr", c).start()

    def a4(c):
        settle(blk_of(c, opposite), ag_recv.at[2, c])
        ag_copy("pp", c).start()

    def a5(c):
        settle(blk_of(c, pl.ds(0, 4)), ag_recv.at[3, c])
        k, cols = piece(c)
        pltpu.make_async_copy(ys.at[k, :, :, cols], y_out.at[k, :, :, cols], yo_sem).start()

    def select(k):
        k2 = lax.rem(k, 2)
        r, c = iota((4 * rows, 8 * rows), 0), iota((4 * rows, 8 * rows), 1)
        sel = (c == (r // 4) * 8 + k2 * 4 + r % 4).astype(F32).astype(BF16)
        pair = xs[k // 2].reshape(8 * rows, width)
        xk[k2] = jnp.dot(sel, pair, preferred_element_type=F32).astype(BF16)

    def hidden(i):
        x = xk[lax.rem(i // blocks, 2)]
        return jax.nn.gelu(jnp.dot(x, wi_buf[lax.rem(i, W_SLOTS)], preferred_element_type=F32)).astype(BF16)

    hooks = {
        0: [(s3, 1, p) for p in range(EARLY, pairs)] + [(select, 1)],
        2: [(s4, 1), (select, 2)],
        3: [(a2, 0)],
        4: [(a3, 0), (select, 3)],
        5: [(a2, 1)],
        6: [(a3, 1), (a4, 0)],
    }

    def wo(i):
        return wo_slot(i)[...]

    def refill(i):
        when(i + 1 + W_SLOTS < steps, (lambda: w_copies(i + 1 + W_SLOTS)[0].start(),))
        when(i + O_SLOTS < steps, (lambda: w_copies(i + O_SLOTS)[1].start(),))

    def ffn_step(t, carry):
        i = 2 * t
        k = i // blocks
        for n in range(2):
            w_copies(i + n + 1)[0].wait()
            w_copies(i + n)[1].wait()
        total = jnp.where(lax.rem(i, blocks) == 0, 0.0, y_acc[...])
        for n in range(2):
            h = hidden(i + n + 1)
            total += jnp.dot(h_buf[n], wo(i + n), preferred_element_type=F32)
            h_buf[1 - n] = h
        y_acc[...] = total
        for n in range(2):
            refill(i + n)

        @pl.when(lax.rem(i, blocks) == blocks - 2)
        def _():
            ys[k, me] = y_acc[...].astype(BF16)
            a1(k)

        for at, todo in hooks.items():
            when(t == at, *todo)
        return carry

    w_copies(0)[0].wait()
    select(0)
    h_buf[0] = hidden(0)
    w_copies(W_SLOTS)[0].start()
    lax.fori_loop(0, steps // 2 - 1, ffn_step, 0)

    w_copies(steps - 1)[0].wait()
    h_buf[1] = hidden(steps - 1)
    a2(2)
    for n in range(2):
        w_copies(steps - 2 + n)[1].wait()
    for c in (experts - 1, experts):
        cols = piece(c)[1]
        total = y_acc[:, cols]
        for n in range(2):
            total += jnp.dot(h_buf[n], wo_slot(steps - 2 + n)[:, cols], preferred_element_type=F32)
        ys[experts - 1, me, :, cols] = total.astype(BF16)
        a1(c)
    a3(2)
    a4(1)
    a5(0)
    a4(2)
    a5(1)
    a2(3)
    a5(2)
    a3(3)
    a2(4)
    a3(4)
    a4(3)
    a4(4)
    a5(3)
    a5(4)

    def finish():
        for p in (pairs - 2, pairs - 1):
            c_copy(p).wait()
        pltpu.make_async_copy(ys, y_out, yo_sem).wait()
        settle(z_peer, z_send.at[0])
        settle(z_all.at[pl.ds(0, 3)], z_send.at[1])
        settle(from_partner, d_send)
        for side, relay in enumerate((relay_r, relay_l)):
            settle(relay.at[0, pl.ds(0, pairs - DIRECT)], a_send.at[side, 0])
            settle(relay.at[1], a_send.at[side, 1])
        settle(from_opp, o_send)
        settle(from_l, b_send.at[0])
        settle(from_r, b_send.at[1])
        for c in range(pieces):
            settle(blk_of(c, pl.ds(0, 7)), ag_send.at[c])

    finish()


def combine_kernel(c_hbm, y_hbm, out_hbm, c_buf, y_buf, out_buf, c_sem, y_sem, out_sem):
    rows = out_hbm.shape[0]
    width = out_hbm.shape[2]
    low = iota((8, width), 0) < 4

    def loads(p):
        slot = lax.rem(p, IN_SLOTS)
        eight = pl.ds(pl.multiple_of(8 * p, 8), 8)
        return (
            pltpu.make_async_copy(y_hbm.at[:, :, eight], y_buf.at[slot], y_sem.at[slot]),
            pltpu.make_async_copy(c_hbm.at[pl.ds(2 * p, 2)], c_buf.at[slot], c_sem.at[slot]),
        )

    def store(b):
        slot = lax.rem(b, OUT_SLOTS)
        return pltpu.make_async_copy(out_buf.at[slot], out_hbm.at[b], out_sem.at[slot])

    def slot_rows(y_ref):
        first, second = [], []
        for kk in range(2):
            for core in range(2):
                for chip in range(4):
                    even = y_ref[2 * kk, chip * 2 + core].astype(F32)
                    odd = y_ref[2 * kk + 1, chip * 2 + core].astype(F32)
                    first.append(jnp.where(low, even, pltpu.roll(odd, 4, 0)))
                    second.append(jnp.where(low, pltpu.roll(even, 4, 0), odd))
        return [jnp.concatenate(tiles, axis=0).astype(BF16) for tiles in (first, second)]

    def step(p, carry):
        for copy in loads(p):
            copy.wait()
        slot = lax.rem(p, IN_SLOTS)
        y = slot_rows(y_buf.at[slot])
        for which in range(2):
            b = 2 * p + which

            @pl.when(b >= OUT_SLOTS)
            def _():
                store(b - OUT_SLOTS).wait()

            mixed = jnp.dot(c_buf[slot, which], y[which], preferred_element_type=F32)
            out_buf[lax.rem(b, OUT_SLOTS)] = mixed.astype(BF16)
            store(b).start()

        @pl.when(p + IN_SLOTS < rows // 2)
        def _():
            for copy in loads(p + IN_SLOTS):
                copy.start()

        return carry

    for p in range(IN_SLOTS):
        for copy in loads(p):
            copy.start()
    lax.fori_loop(0, rows // 2, step, 0)
    for b in range(rows - OUT_SLOTS, rows):
        store(b).wait()


def solution(mesh):
    def shard_body(tok, lens, phi, gain, w_in, w_out):
        rows, tokens, width = tok.shape
        experts, _, ff = w_in.shape
        slots = phi.shape[1]
        pairs = rows // 2
        any_spec = pl.BlockSpec(memory_space=pl.ANY)
        smem = pl.BlockSpec(memory_space=pltpu.SMEM)
        dma = pltpu.SemaphoreType.DMA
        blk = (16, width)
        c, y = pl.pallas_call(
            route_kernel,
            out_shape=(
                jax.ShapeDtypeStruct((rows, tokens, slots), BF16),
                jax.ShapeDtypeStruct((experts, 8, 4 * rows, width), BF16),
            ),
            in_specs=[smem, smem, pl.BlockSpec(memory_space=pltpu.VMEM), any_spec, any_spec, any_spec],
            out_specs=(any_spec, any_spec),
            scratch_shapes=[
                pltpu.VMEM((width, slots), BF16),
                pltpu.VMEM((2, slots, tokens), BF16),
                pltpu.VMEM((2, slots, width), F32),
                pltpu.VMEM((2, 2, tokens, slots), BF16),
                pltpu.VMEM((2, 2, 4, pairs) + blk, BF16),
                pltpu.VMEM((2, 4, pairs) + blk, BF16),
                pltpu.VMEM((2, pairs, 16, width // 2), BF16),
                pltpu.VMEM((2, pairs, 16, width // 2), BF16),
                pltpu.VMEM((2, pairs) + blk, BF16),
                pltpu.VMEM((2, pairs) + blk, BF16),
                pltpu.VMEM((DIRECT,) + blk, BF16),
                pltpu.VMEM((2, pairs) + blk, BF16),
                pltpu.VMEM((rows, slots), F32),
                pltpu.VMEM((rows, slots), F32),
                pltpu.VMEM((rows, slots), F32),
                pltpu.VMEM((4, rows, slots), F32),
                pltpu.VMEM((rows, slots), F32),
                pltpu.VMEM((2, 4 * rows, width), BF16),
                pltpu.VMEM((2, 4 * rows, F_BLOCK), BF16),
                pltpu.VMEM((4 * rows, width), F32),
                pltpu.VMEM((experts, 8, 4 * rows, width), BF16),
                pltpu.VMEM((W_SLOTS, width, F_BLOCK), BF16),
                pltpu.VMEM((W_SLOTS * F_BLOCK + max(F_BLOCK, TOK_SLOTS * tokens), width), BF16),
                dma((TOK_SLOTS,)), dma((W_SLOTS,)), dma((O_SLOTS,)), dma((2,)), dma, dma((2,)), dma((2,)),
                dma, dma((2, pairs)), dma((2, 2)), dma((2, 2, pairs)), dma((2,)), dma((2, 2)), dma, dma, dma((experts + 1,)), dma((4, experts + 1)),
            ],
            compiler_params=pltpu.CompilerParams(
                collective_id=0, has_side_effects=True, vmem_limit_bytes=67_000_000
            ),
            name="route",
        )(lens, gain, phi, tok, w_in, w_out)
        return pl.pallas_call(
            combine_kernel,
            out_shape=jax.ShapeDtypeStruct(tok.shape, BF16),
            in_specs=[any_spec, any_spec],
            out_specs=any_spec,
            scratch_shapes=[
                pltpu.VMEM((IN_SLOTS, 2, tokens, slots), BF16),
                pltpu.VMEM((IN_SLOTS, experts, 8, 8, width), BF16),
                pltpu.VMEM((OUT_SLOTS, tokens, width), BF16),
                dma((IN_SLOTS,)), dma((IN_SLOTS,)), dma((OUT_SLOTS,)),
            ],
            compiler_params=pltpu.CompilerParams(vmem_limit_bytes=67_000_000),
            name="combine",
        )(c, y)

    return jax.shard_map(
        shard_body,
        mesh=mesh,
        in_specs=(P("data", "seq", None), P("data"), P(None, None), P(None), P("seq", None, None), P("seq", None, None)),
        out_specs=P("data", "seq", None),
        check_vma=False,
    )
```

```python
import functools

import jax
import jax.numpy as jnp
from jax import lax
from jax.experimental import pallas as pl
from jax.experimental.pallas import tpu as pltpu
from jax.sharding import PartitionSpec as P

MESH = pl.DeviceIdType.MESH
F32, BF16 = jnp.float32, jnp.bfloat16
TOK_SLOTS = 4
W_SLOTS = 6
O_SLOTS = W_SLOTS + 1
EARLY = 4
F_BLOCK = 1280
ROW_TILE = 128
IN_SLOTS = 3
OUT_SLOTS = 4


def iota(shape, dim):
    return lax.broadcasted_iota(jnp.int32, shape, dim)


def route_kernel(
    lens, gain, phi, tok, w_in, w_out, c_out, y_out,
    phin, wt_buf, s_f32, c_buf, part, from_partner, relay, from_l, from_r, xs, z_own, z_peer, z_chip, z_all, z_tot,
    xk, h_buf, ys, wi_buf, wo_buf,
    phi_sem, tok_sem, wi_sem, wo_sem, c_sem, yo_sem, z_send, z_recv,
    d_send, d_recv, a_send, a_recv, b_send, b_recv, o_send, o_recv, ag_send, ag_recv,
):
    rows, tokens, width = tok.shape
    experts, _, ff = w_in.shape
    slots = phi.shape[1]
    pairs = rows // 2
    blocks = ff // F_BLOCK
    steps = experts * blocks
    me = lax.axis_index("seq")
    chip, core = me // 2, lax.rem(me, 2)

    def dev(chip_step, flip=0):
        other = lax.rem(chip + chip_step, 4)
        return other * 2 + (1 - core if flip else core)

    left, right, opposite, partner = dev(3), dev(1), dev(2), dev(0, 1)
    c_left, c_right, c_opp = lax.rem(chip + 3, 4), lax.rem(chip + 1, 4), lax.rem(chip + 2, 4)

    barrier = pltpu.get_barrier_semaphore()
    for step in range(1, 8):
        peer = lax.rem(me + step, 8)
        pl.semaphore_signal(barrier, inc=1, device_id={"seq": peer}, device_id_type=MESH)

    def tok_slot(b):
        first = W_SLOTS * F_BLOCK + lax.rem(b, TOK_SLOTS) * tokens
        return wo_buf.at[pl.ds(pl.multiple_of(first, 256), tokens)]

    def wo_slot(i):
        return wo_buf.at[pl.ds(pl.multiple_of(lax.rem(i, O_SLOTS) * F_BLOCK, 256), F_BLOCK)]

    def tok_copy(b):
        return pltpu.make_async_copy(tok.at[b], tok_slot(b), tok_sem.at[lax.rem(b, TOK_SLOTS)])

    def w_copies(i):
        e, f = i // blocks, lax.rem(i, blocks)
        cols = pl.ds(pl.multiple_of(f * F_BLOCK, F_BLOCK), F_BLOCK)
        i_slot = lax.rem(i, W_SLOTS)
        return (
            pltpu.make_async_copy(w_in.at[e, :, cols], wi_buf.at[i_slot], wi_sem.at[i_slot]),
            pltpu.make_async_copy(w_out.at[e, cols, :], wo_slot(i), wo_sem.at[lax.rem(i, O_SLOTS)]),
        )

    phi_copy = pltpu.make_async_copy(phi, phin, phi_sem)
    tok_copy(0).start()
    phi_copy.start()
    tok_copy(1).start()

    gain_s = gain[0]
    phi_copy.wait()
    phi_f32 = phin[...].astype(F32)
    col_inv = lax.rsqrt(jnp.sum(phi_f32 * phi_f32, axis=0, keepdims=True) + 1e-6)
    phi_n = (phi_f32 * (gain_s * col_inv)).astype(BF16)
    src, dst = iota((slots, slots), 0), iota((slots, slots), 1)
    kk, hh, cc, rest = dst // 64, (dst // 32) % 2, (dst // 8) % 4, dst % 8
    perm = (src == cc * 32 + hh * 16 + kk * 8 + rest).astype(F32).astype(BF16)
    phin[...] = jnp.dot(phi_n, perm, preferred_element_type=F32).astype(BF16)

    for b in range(2, TOK_SLOTS):
        tok_copy(b).start()

    def c_copy(p):
        slot = lax.rem(p, 2)
        return pltpu.make_async_copy(c_buf.at[slot], c_out.at[pl.ds(2 * p, 2)], c_sem.at[slot])

    def pack_pair(p):
        for g in range(16):
            eight = pl.ds(g * 8, 8)
            both = jnp.concatenate([s_f32[0, eight, :], s_f32[1, eight, :]], axis=0)
            part[g // 8, (g // 4) % 2, g % 4, p] = both.astype(BF16)

    def one_row(p, which):
        b = 2 * p + which
        x_ref = tok_slot(b)
        length = lens[b]
        z_row = jnp.zeros((1, slots), F32)
        for r in range(tokens // ROW_TILE):
            tile = pl.ds(r * ROW_TILE, ROW_TILE)
            x = x_ref[tile, :].astype(F32)
            inv = lax.rsqrt(jnp.sum(x * x, axis=-1, keepdims=True) + 1e-6)
            logits = jnp.dot((x * inv).astype(BF16), phin[...], preferred_element_type=F32)
            e = jnp.exp(logits - gain_s)
            pos = me * tokens + r * ROW_TILE + iota((ROW_TILE, slots), 0)
            valid = pos < length
            total = jnp.sum(e, axis=-1, keepdims=True)
            c_buf[lax.rem(p, 2), which, tile, :] = jnp.where(valid, e / total, 0.0).astype(BF16)
            w = jnp.where(valid, e, 0.0)
            z_row += jnp.sum(w, axis=0, keepdims=True)
            wt_buf[which, :, tile] = w.T.astype(BF16)
        z_own[pl.ds(b, 1), :] = z_row
        s_f32[which] = jnp.dot(wt_buf[which], x_ref[...], preferred_element_type=F32)

    def remote(src_ref, dst_ref, send, recv, to):
        return pltpu.make_async_remote_copy(
            src_ref=src_ref, dst_ref=dst_ref, send_sem=send, recv_sem=recv, device_id={"seq": to}, device_id_type=MESH
        )

    lo_cols, hi_cols = pl.ds(0, width // 2), pl.ds(width // 2, width // 2)

    def settle(ref, sem):
        pltpu.make_async_copy(ref, ref, sem).wait()

    def d2d(kk, p):
        return remote(part.at[kk, 1 - core, :, p], from_partner.at[kk, :, p], d_send, d_recv.at[kk, p], partner)

    def rs_copy(kind, kk, p):
        mine = part.at[kk, core]
        to_right = kind[1] == "p"
        side, to = (0, right) if to_right else (1, left)
        if kind[0] == "a":
            cols = lo_cols if to_right else hi_cols
            return remote(mine.at[c_opp, p, :, cols], relay.at[kk, p, :, cols], a_send.at[side, kk], a_recv.at[side, kk, p], to)
        cols = hi_cols if kind in ("bp0", "bm1") else lo_cols
        c, inbox = (c_right, from_l) if to_right else (c_left, from_r)
        return remote(mine.at[c, p, :, cols], inbox.at[kk, p, :, cols], b_send.at[side], b_recv.at[side, kk], to)

    def chip_sum(kk, p):
        d2d(kk, p).wait_recv()
        for c in range(4):
            total = part[kk, core, c, p].astype(F32) + from_partner[kk, c, p].astype(F32)
            part[kk, core, c, p] = total.astype(BF16)

    def s2(kk, p):
        chip_sum(kk, p)
        for kind in ("ap", "am", "bp0", "bm0"):
            rs_copy(kind, kk, p).start()

    def s2_direct(p):
        chip_sum(0, p)
        mine = part.at[0, core]
        remote(mine.at[c_opp, p], relay.at[0, p], o_send, o_recv, opposite).start()
        remote(mine.at[c_right, p], from_l.at[0, p], b_send.at[0], b_recv.at[0, 0], right).start()
        remote(mine.at[c_left, p], from_r.at[0, p], b_send.at[1], b_recv.at[1, 0], left).start()

    def s3(kk, p):
        for kind, then, c, cols in (("ap", "bp1", c_right, lo_cols), ("am", "bm1", c_left, hi_cols)):
            rs_copy(kind, kk, p).wait_recv()
            total = part[kk, core, c, p, :, cols].astype(F32) + relay[kk, p, :, cols].astype(F32)
            part[kk, core, c, p, :, cols] = total.astype(BF16)
            rs_copy(then, kk, p).start()

    def s4(kk):
        lane0 = kk * 64 + core * 32 + chip * 8
        pick = iota((16, slots), 1) == lane0 + iota((16, slots), 0) % 8
        cols = []
        for p in range(pairs):
            z16 = jnp.concatenate([jnp.broadcast_to(z_tot[b : b + 1, :], (8, slots)) for b in (2 * p, 2 * p + 1)], axis=0)
            cols.append(jnp.sum(jnp.where(pick, z16, 0.0), axis=1, keepdims=True))
        settle(from_l.at[kk], b_recv.at[0, kk])
        settle(from_r.at[kk], b_recv.at[1, kk])
        if kk == 0:
            settle(relay.at[0, pairs - 1], o_recv)
        for p in range(pairs):
            total = part[kk, core, chip, p].astype(F32) + from_l[kk, p].astype(F32) + from_r[kk, p].astype(F32)
            if kk == 0 and p == pairs - 1:
                total += relay[0, p].astype(F32)
            xs[kk, p] = (total / cols[p]).astype(BF16)

    def z_pair():
        return remote(z_own, z_peer, z_send.at[0], z_recv.at[0], partner)

    def z_chips():
        return [remote(z_chip, z_all.at[chip], z_send.at[1], z_recv.at[1], to) for to in (right, left, opposite)]

    def when(condition, *todo):
        @pl.when(condition)
        def _():
            for f, *args in todo:
                f(*args)

    def pair_step(p, carry):
        when(p >= 2, (lambda: c_copy(p - 2).wait(),))
        for which in range(2):
            tok_copy(2 * p + which).wait()
        for which in range(2):
            one_row(p, which)
        pack_pair(p)
        when(p == pairs - 1, (lambda: z_pair().start(),))
        d2d(0, p).start()
        d2d(1, p).start()
        c_copy(p).start()
        for which in range(2):
            b = 2 * p + TOK_SLOTS + which
            when(b < rows, (lambda b=b: tok_copy(b).start(),))
        for n in range(2 * W_SLOTS):
            when(p == n * pairs // (2 * W_SLOTS), (w_copies(n // 2)[n % 2].start,))
        when(p >= 1, (s2, 0, p - 1))
        when(p >= 3, (s3, 0, p - 3))
        when((p >= 1) & (p <= EARLY), (s2, 1, p - 1))
        when(p >= pairs - EARLY, (s3, 1, p - (pairs - EARLY)))
        return carry

    pl.semaphore_wait(barrier, 7)
    lax.fori_loop(0, pairs, pair_step, 0)
    w_copies(W_SLOTS)[1].start()
    z_pair().wait_recv()
    z_chip[...] = z_own[...] + z_peer[...]
    for copy in z_chips():
        copy.start()
    s2_direct(pairs - 1)
    s3(0, pairs - 3)
    s3(0, pairs - 2)
    for p in range(EARLY, pairs):
        s2(1, p)
    settle(z_all.at[pl.ds(0, 3)], z_recv.at[1])
    z = z_chip[...]
    for c in (c_right, c_left, c_opp):
        z += z_all[c]
    z_tot[...] = z
    s4(0)

    half = 2 * rows
    lo, hi = pl.ds(0, half), pl.ds(half, half)

    split = 3 * (width // 5)
    pieces = 2 + experts - 1

    def piece(c):
        if isinstance(c, int) and c >= experts - 1:
            return experts - 1, pl.ds(0, split) if c == experts - 1 else pl.ds(split, width - split)
        return c, pl.ds(0, width)

    def blk_of(c, d, part_rows=pl.ds(0, 4 * rows)):
        k, cols = piece(c)
        return ys.at[k, d, part_rows, cols]

    def ag_copy(kind, c):
        src_blk, part_rows, to, arrival = {
            "rp": (me, lo, right, 0),
            "lm": (me, hi, left, 0),
            "rm": (me, hi, right, 1),
            "lp": (me, lo, left, 1),
            "fr": (left, lo, right, 2),
            "fl": (right, hi, left, 2),
            "po": (me, None, partner, 3),
            "pl": (left, None, partner, 3),
            "pr": (right, None, partner, 3),
            "pp": (opposite, None, partner, 3),
        }[kind]
        ref = blk_of(c, src_blk) if part_rows is None else blk_of(c, src_blk, part_rows)
        return remote(ref, ref, ag_send.at[c], ag_recv.at[arrival, c], to)

    def a1(c):
        for kind in ("rp", "lm", "rm", "lp", "po"):
            ag_copy(kind, c).start()

    def a2(c):
        settle(blk_of(c, left), ag_recv.at[0, c])
        ag_copy("fr", c).start()
        ag_copy("fl", c).start()

    def a3(c):
        settle(blk_of(c, left), ag_recv.at[1, c])
        ag_copy("pl", c).start()
        ag_copy("pr", c).start()

    def a4(c):
        settle(blk_of(c, opposite), ag_recv.at[2, c])
        ag_copy("pp", c).start()

    def a5(c):
        settle(blk_of(c, pl.ds(0, 4)), ag_recv.at[3, c])
        k, cols = piece(c)
        pltpu.make_async_copy(ys.at[k, :, :, cols], y_out.at[k, :, :, cols], yo_sem).start()

    y_acc = s_f32.at[0, pl.ds(0, 4 * rows)]

    def select(k):
        k2 = lax.rem(k, 2)
        r, c = iota((4 * rows, 8 * rows), 0), iota((4 * rows, 8 * rows), 1)
        sel = (c == (r // 4) * 8 + k2 * 4 + r % 4).astype(F32).astype(BF16)
        pair = xs[k // 2].reshape(8 * rows, width)
        xk[k2] = jnp.dot(sel, pair, preferred_element_type=F32).astype(BF16)

    def hidden(i):
        x = xk[lax.rem(i // blocks, 2)]
        return jax.nn.gelu(jnp.dot(x, wi_buf[lax.rem(i, W_SLOTS)], preferred_element_type=F32)).astype(BF16)

    hooks = {
        0: [(s3, 1, p) for p in range(EARLY, pairs)] + [(select, 1)],
        2: [(s4, 1), (select, 2)],
        3: [(a2, 0)],
        4: [(a3, 0), (select, 3)],
        5: [(a2, 1)],
        6: [(a3, 1), (a4, 0)],
    }

    def wo(i):
        return wo_slot(i)[...]

    def ffn_step(early, t, carry):
        i = 2 * t
        k = i // blocks
        for n in range(2):
            w_copies(i + n + 1)[0].wait()
            w_copies(i + n)[1].wait()
        total = jnp.where(lax.rem(i, blocks) == 0, 0.0, y_acc[...])
        for n in range(2):
            h = hidden(i + n + 1)
            total += jnp.dot(h_buf[n], wo(i + n), preferred_element_type=F32)
            h_buf[1 - n] = h
            if early and n == 0:
                w_copies(i + 1 + W_SLOTS)[0].start()
                w_copies(i + O_SLOTS)[1].start()
        y_acc[...] = total
        if early:
            when(i + 2 + W_SLOTS < steps, (lambda: w_copies(i + 2 + W_SLOTS)[0].start(),))
            when(i + 1 + O_SLOTS < steps, (lambda: w_copies(i + 1 + O_SLOTS)[1].start(),))

        @pl.when(lax.rem(i, blocks) == blocks - 2)
        def _():
            ys[k, me] = y_acc[...].astype(BF16)
            a1(k)

        for at, todo in hooks.items():
            when(t == at, *todo)
        return carry

    w_copies(0)[0].wait()
    select(0)
    h_buf[0] = hidden(0)
    w_copies(W_SLOTS)[0].start()
    fetching = (steps - O_SLOTS + 1) // 2
    lax.fori_loop(0, fetching, functools.partial(ffn_step, True), 0)
    lax.fori_loop(fetching, steps // 2 - 1, functools.partial(ffn_step, False), 0)

    w_copies(steps - 1)[0].wait()
    h_buf[1] = hidden(steps - 1)
    a2(2)
    for n in range(2):
        w_copies(steps - 2 + n)[1].wait()
    for c in (experts - 1, experts):
        cols = piece(c)[1]
        total = y_acc[:, cols]
        for n in range(2):
            total += jnp.dot(h_buf[n], wo_slot(steps - 2 + n)[:, cols], preferred_element_type=F32)
        ys[experts - 1, me, :, cols] = total.astype(BF16)
        a1(c)
    a3(2)
    a4(1)
    a5(0)
    a4(2)
    a5(1)
    a2(3)
    a5(2)
    a3(3)
    a2(4)
    a3(4)
    a4(3)
    a4(4)
    a5(3)
    a5(4)

    def finish():
        for p in (pairs - 2, pairs - 1):
            c_copy(p).wait()
        pltpu.make_async_copy(ys, y_out, yo_sem).wait()
        settle(z_peer, z_send.at[0])
        settle(z_all.at[pl.ds(0, 3)], z_send.at[1])
        settle(from_partner, d_send)
        for side, cols in enumerate((lo_cols, hi_cols)):
            settle(relay.at[0, pl.ds(0, pairs - 1), :, cols], a_send.at[side, 0])
            settle(relay.at[1, :, :, cols], a_send.at[side, 1])
        settle(relay.at[0, pairs - 1], o_send)
        settle(from_l, b_send.at[0])
        settle(from_r, b_send.at[1])
        for c in range(pieces):
            settle(blk_of(c, pl.ds(0, 7)), ag_send.at[c])

    finish()


def combine_kernel(c_hbm, y_hbm, out_hbm, c_buf, y_buf, out_buf, c_sem, y_sem, out_sem):
    rows = out_hbm.shape[0]
    width = out_hbm.shape[2]
    low = iota((8, width), 0) < 4

    def loads(p):
        slot = lax.rem(p, IN_SLOTS)
        eight = pl.ds(pl.multiple_of(8 * p, 8), 8)
        return (
            pltpu.make_async_copy(y_hbm.at[:, :, eight], y_buf.at[slot], y_sem.at[slot]),
            pltpu.make_async_copy(c_hbm.at[pl.ds(2 * p, 2)], c_buf.at[slot], c_sem.at[slot]),
        )

    def store(b):
        slot = lax.rem(b, OUT_SLOTS)
        return pltpu.make_async_copy(out_buf.at[slot], out_hbm.at[b], out_sem.at[slot])

    def slot_rows(y_ref):
        first, second = [], []
        for kk in range(2):
            for core in range(2):
                for chip in range(4):
                    even = y_ref[2 * kk, chip * 2 + core].astype(F32)
                    odd = y_ref[2 * kk + 1, chip * 2 + core].astype(F32)
                    first.append(jnp.where(low, even, pltpu.roll(odd, 4, 0)))
                    second.append(jnp.where(low, pltpu.roll(even, 4, 0), odd))
        return [jnp.concatenate(tiles, axis=0).astype(BF16) for tiles in (first, second)]

    def step(p, carry):
        for copy in loads(p):
            copy.wait()
        slot = lax.rem(p, IN_SLOTS)
        y = slot_rows(y_buf.at[slot])
        for which in range(2):
            b = 2 * p + which

            @pl.when(b >= OUT_SLOTS)
            def _():
                store(b - OUT_SLOTS).wait()

            mixed = jnp.dot(c_buf[slot, which], y[which], preferred_element_type=F32)
            out_buf[lax.rem(b, OUT_SLOTS)] = mixed.astype(BF16)
            store(b).start()

        @pl.when(p + IN_SLOTS < rows // 2)
        def _():
            for copy in loads(p + IN_SLOTS):
                copy.start()

        return carry

    for p in range(IN_SLOTS):
        for copy in loads(p):
            copy.start()
    lax.fori_loop(0, rows // 2, step, 0)
    for b in range(rows - OUT_SLOTS, rows):
        store(b).wait()


def solution(mesh):
    def shard_body(tok, lens, phi, gain, w_in, w_out):
        rows, tokens, width = tok.shape
        experts, _, ff = w_in.shape
        slots = phi.shape[1]
        pairs = rows // 2
        any_spec = pl.BlockSpec(memory_space=pl.ANY)
        smem = pl.BlockSpec(memory_space=pltpu.SMEM)
        dma = pltpu.SemaphoreType.DMA
        blk = (16, width)
        c, y = pl.pallas_call(
            route_kernel,
            out_shape=(
                jax.ShapeDtypeStruct((rows, tokens, slots), BF16),
                jax.ShapeDtypeStruct((experts, 8, 4 * rows, width), BF16),
            ),
            in_specs=[smem, smem, any_spec, any_spec, any_spec, any_spec],
            out_specs=(any_spec, any_spec),
            scratch_shapes=[
                pltpu.VMEM((width, slots), BF16),
                pltpu.VMEM((2, slots, tokens), BF16),
                pltpu.VMEM((2, slots, width), F32),
                pltpu.VMEM((2, 2, tokens, slots), BF16),
                pltpu.VMEM((2, 2, 4, pairs) + blk, BF16),
                pltpu.VMEM((2, 4, pairs) + blk, BF16),
                pltpu.VMEM((2, pairs) + blk, BF16),
                pltpu.VMEM((2, pairs) + blk, BF16),
                pltpu.VMEM((2, pairs) + blk, BF16),
                pltpu.VMEM((2, pairs) + blk, BF16),
                pltpu.VMEM((rows, slots), F32),
                pltpu.VMEM((rows, slots), F32),
                pltpu.VMEM((rows, slots), F32),
                pltpu.VMEM((4, rows, slots), F32),
                pltpu.VMEM((rows, slots), F32),
                pltpu.VMEM((2, 4 * rows, width), BF16),
                pltpu.VMEM((2, 4 * rows, F_BLOCK), BF16),
                pltpu.VMEM((experts, 8, 4 * rows, width), BF16),
                pltpu.VMEM((W_SLOTS, width, F_BLOCK), BF16),
                pltpu.VMEM((W_SLOTS * F_BLOCK + max(F_BLOCK, TOK_SLOTS * tokens), width), BF16),
                dma, dma((TOK_SLOTS,)), dma((W_SLOTS,)), dma((O_SLOTS,)), dma((2,)), dma, dma((2,)), dma((2,)),
                dma, dma((2, pairs)), dma((2, 2)), dma((2, 2, pairs)), dma((2,)), dma((2, 2)), dma, dma, dma((experts + 1,)), dma((4, experts + 1)),
            ],
            compiler_params=pltpu.CompilerParams(
                collective_id=0, has_side_effects=True, vmem_limit_bytes=67_000_000
            ),
            name="route",
        )(lens, gain, phi, tok, w_in, w_out)
        return pl.pallas_call(
            combine_kernel,
            out_shape=jax.ShapeDtypeStruct(tok.shape, BF16),
            in_specs=[any_spec, any_spec],
            out_specs=any_spec,
            scratch_shapes=[
                pltpu.VMEM((IN_SLOTS, 2, tokens, slots), BF16),
                pltpu.VMEM((IN_SLOTS, experts, 8, 8, width), BF16),
                pltpu.VMEM((OUT_SLOTS, tokens, width), BF16),
                dma((IN_SLOTS,)), dma((IN_SLOTS,)), dma((OUT_SLOTS,)),
            ],
            compiler_params=pltpu.CompilerParams(vmem_limit_bytes=67_000_000),
            name="combine",
        )(c, y)

    return jax.shard_map(
        shard_body,
        mesh=mesh,
        in_specs=(P("data", "seq", None), P("data"), P(None, None), P(None), P("seq", None, None), P("seq", None, None)),
        out_specs=P("data", "seq", None),
        check_vma=False,
    )
```
